512 devices in a mesh: section: 8 (over z_hi, x), dp: 64 (over z_lo, y, core).
Axes of the slice: x: 4, y: 8, z: 8 (z_hi: 2, z_lo: 4; z = z_hi * 4 + z_lo), core: 2. Of those that a mesh axis runs over, the one named last changes fastest.
Arguments:
- inputs: bfloat16 [8192, 8192], P('dp', 'section'), may hold values from -6 to 6
- cotangent: bfloat16 [8192, 8192], P('dp', 'section'), may hold values from -6 to 6
- weights: bfloat16 [8, 64, 8192], P('section'), may hold values from -0.0625 to 0.0625
- momentum: bfloat16 [8, 64, 64, 8192], P('section', 'dp'), may hold values from -6 to 6
- keep_index: int32 [8, 64, 128, 32], P('section', 'dp'), may hold values from 0 to 4095, as said below
Outputs:
- momentum_out: bfloat16 [8, 64, 64, 8192], P('section', 'dp')
- update: bfloat16 [8, 64, 64, 8192], P('section', 'dp')
The draws below stay inside these ranges and needn't reach their ends.
Inputs may be any that keep to these rules, and one draw needn't show every extreme that they name: `keep_index`: the 32 positions of one block of one replica and layer are all different.
All inputs are finite; a program needn't handle non-finite values.
Results may differ from the reference program's by a relative error of at most 0.0095.
Values may be sent and summed in bfloat16 or wider, within the bound.
No kernel may reach another device: no remote copies, remote signals or barrier semaphores. Data moves between devices by JAX's collectives and lax.ppermute only.
A program may use at most 64 MiB of HBM per device.

```python
import math
import jax
import jax.numpy as jnp
from jax import lax

D = 8192
COLS = 64
K = 32
LAYERS = 8
REPLICAS = 64
TOKENS = 8192
GROUPS = 128


def draw_keep_index(key, part):
    sub_keys = jax.random.split(key, LAYERS * REPLICAS)

    def draw_rows(sub_key):
        scores = jax.random.randint(sub_key, (GROUPS, 4096), 0, 2 ** 18, dtype=jnp.int32)
        scores = scores * 4096 + jnp.arange(4096, dtype=jnp.int32)[None, :]
        return lax.top_k(scores, K)[1].astype(jnp.int32)
    return lax.map(draw_rows, sub_keys).reshape(LAYERS, REPLICAS, GROUPS, K)


def steps_of(rng, shape, cuts, low, top_value):
    factor_of = 1.0
    for dim, blocks in cuts:
        draws = jax.random.uniform(jax.random.fold_in(jax.random.fold_in(rng, 6), dim), (blocks,), jnp.float32, low / len(cuts), top_value / len(cuts))
        factor_of = factor_of * jnp.repeat(jnp.exp(draws), shape[dim] // blocks).reshape((-1,) + (1,) * (len(shape) - 1 - dim))
    return factor_of


def bell_draw(rng, dims, deviation, reach, shards=(), held_as=jnp.bfloat16):
    values = deviation * jax.random.normal(rng, dims, jnp.float32)
    if shards:
        values = values * steps_of(rng, dims, shards, -0.22, 0.18)
    return jnp.clip(values, -reach, reach).astype(held_as)


def setup_inputs(seed: int = 0) -> dict:
    key_of = jax.random.split(jax.random.key(seed), 6)
    inputs = bell_draw(key_of[0], (TOKENS, D), 1.0, 6.0, ((0, 64), (1, 8)))
    cotangent = bell_draw(key_of[1], (TOKENS, D), 1.0, 6.0, ((0, 64), (1, 8)))
    weights = bell_draw(key_of[2], (LAYERS, COLS, D), D ** -0.5, 0.0625, ((0, 8),))
    momentum = bell_draw(key_of[3], (LAYERS, REPLICAS, COLS, D), 1.0, 6.0, ((0, 8), (1, 64)))
    keep_index = draw_keep_index(jax.random.fold_in(key_of[5], 71), 0)
    return {"inputs": inputs, "cotangent": cotangent, "weights": weights, "momentum": momentum, "keep_index": keep_index}


DECAY = 0.999

def dct_basis(length):
    freq = jnp.arange(length, dtype=jnp.float32)[:, None]
    position = jnp.arange(length, dtype=jnp.float32)[None, :]
    dct_table = jnp.cos(math.pi * (position + 0.5) * freq / length) * math.sqrt(2.0 / length)
    return jnp.where(freq == 0, dct_table * math.sqrt(0.5), dct_table)

def forward_groups(field_in, dct_table):
    row_count, columns = field_in.shape[-2:]
    blocks = field_in.reshape(field_in.shape[:-2] + (row_count // 64, 64, columns // 64, 64))
    coeffs = jnp.einsum('kn,...anbm,jm->...akbj', dct_table, blocks, dct_table, precision=lax.Precision.HIGHEST)
    return coeffs.reshape(field_in.shape[:-2] + (-1,))

def inverse_groups(flat_in, dct_table, row_count, columns):
    blocks = flat_in.reshape(flat_in.shape[:-1] + (row_count // 64, 64, columns // 64, 64))
    field_out = jnp.einsum('kn,...akbj,jm->...anbm', dct_table, blocks, dct_table, precision=lax.Precision.HIGHEST)
    return field_out.reshape(flat_in.shape[:-1] + (row_count, columns))

def group_offsets(position, col_groups):
    group_id = jnp.arange(position.shape[-2], dtype=jnp.int32)[:, None]
    return group_id // col_groups * (4096 * col_groups) + position // 64 * (64 * col_groups) + group_id % col_groups * 64 + position % 64

def silu_slope(pre_act):
    sigma_h = jax.nn.sigmoid(pre_act)
    return sigma_h * (1.0 + pre_act * (1.0 - sigma_h))

def reference(inputs, cotangent, weights, momentum, keep_index):
    layers = weights.shape[0]
    replicas = momentum.shape[1]
    row_count, columns = (weights.shape[1], weights.shape[2])
    dct_table = dct_basis(64)
    activation = inputs
    saved_acts = []
    for layer_idx in range(layers):
        weight = weights[layer_idx]
        pre_act = jnp.dot(activation, weight.T, preferred_element_type=jnp.float32)
        gated_act = jax.nn.silu(pre_act).astype(jnp.bfloat16)
        saved_acts.append((activation, gated_act, pre_act))
        activation = (activation.astype(jnp.float32) + jnp.dot(gated_act, weight, preferred_element_type=jnp.float32)).astype(jnp.bfloat16)

    def by_replica(value):
        return value.astype(jnp.float32).reshape(replicas, -1, value.shape[-1])
    grad_in = cotangent
    moment_list = [None] * layers
    update_list = [None] * layers
    for layer_idx in reversed(range(layers)):
        activation, gated_act, pre_act = saved_acts[layer_idx]
        weight = weights[layer_idx]
        errors = jnp.dot(grad_in, weight.T, preferred_element_type=jnp.float32)
        deltas = (errors * silu_slope(pre_act)).astype(jnp.bfloat16)
        grad_total = jnp.einsum('rtc,rtd->rcd', by_replica(gated_act), by_replica(grad_in), precision=lax.Precision.HIGHEST)
        grad_total = grad_total + jnp.einsum('rtc,rtd->rcd', by_replica(deltas), by_replica(activation), precision=lax.Precision.HIGHEST)
        grad_in = (grad_in.astype(jnp.float32) + jnp.dot(deltas, weight, preferred_element_type=jnp.float32)).astype(jnp.bfloat16)
        momentum_new = DECAY * momentum[layer_idx].astype(jnp.float32) + grad_total
        coeffs = forward_groups(momentum_new, dct_table)
        offsets = group_offsets(keep_index[layer_idx], columns // 64).reshape(replicas, -1)
        kept_values = jnp.take_along_axis(coeffs, offsets, axis=1)
        replica_ids = jnp.arange(replicas, dtype=jnp.int32)[:, None] + jnp.zeros_like(offsets)
        sparse = jnp.zeros_like(coeffs).at[replica_ids, offsets].add(kept_values)
        own_field = inverse_groups(sparse, dct_table, row_count, columns)
        moment_list[layer_idx] = (momentum_new - own_field).astype(jnp.bfloat16)
        summed = lax.optimization_barrier(jnp.sum(sparse, axis=0))
        combined = inverse_groups(summed, dct_table, row_count, columns).astype(jnp.bfloat16)
        update_list[layer_idx] = jnp.broadcast_to(combined[None], (replicas, row_count, columns))
    return (jnp.stack(moment_list), jnp.stack(update_list))
```

```python
import math

import jax
import jax.numpy as jnp
from jax import lax
from jax.sharding import Mesh, PartitionSpec as P

DECAY = 0.999
S = ("zh", "x")
CHIP = ("zl", "y")
DP = ("zl", "y", "core")
F32 = jnp.float32
BF = jnp.bfloat16


def a2a(value, axis):
    return lax.all_to_all(value, axis, 0, 0, tiled=True)


def swap_cores(value):
    return lax.ppermute(value, "core", [(0, 1), (1, 0)])


def mm(a, b, dims):
    return lax.dot_general(a, b, (dims, ((), ())), preferred_element_type=F32)


def split(value):
    high = value.astype(BF)
    return high, (value - high.astype(F32)).astype(BF)


def dct_basis(length):
    freq = jnp.arange(length, dtype=F32)[:, None]
    position = jnp.arange(length, dtype=F32)[None, :]
    table = jnp.cos(math.pi * (position + 0.5) * freq / length) * math.sqrt(2.0 / length)
    return jnp.where(freq == 0, table * math.sqrt(0.5), table)


def silu_slope(h):
    s = jax.nn.sigmoid(h)
    return s * (1.0 + h * (1.0 - s))


def local(inputs, cotangent, weights, momentum, keep_index):
    ns = lax.axis_size(S)
    nd = lax.axis_size(DP)
    core = lax.axis_index("core")
    weight = weights[0]
    rows, width = weight.shape
    cols = width // ns
    tok = inputs.shape[0]
    part = tok // ns
    full = ns * rows
    groups = width // 64
    own = groups // nd

    half = lax.dynamic_slice_in_dim(weight, core * (rows // 2), rows // 2, 0)
    mine = a2a(half.reshape(rows // 2, ns, cols).transpose(1, 0, 2), S)
    other = swap_cores(mine)
    w = jnp.concatenate(
        [jnp.where(core == 0, mine, other), jnp.where(core == 0, other, mine)], axis=1
    ).reshape(full, cols)

    both = jnp.concatenate([inputs, cotangent], axis=0)
    proj = mm(both, w, ((1,), (1,))).astype(BF)
    gram = mm(w, w, ((1,), (1,))).astype(BF)
    packed = []
    for k in range(ns // 2):
        m = ns - 1 - k
        packed.append(
            jnp.concatenate(
                [
                    gram[m * rows : (m + 1) * rows, (m + 1) * rows :],
                    gram[k * rows : (k + 1) * rows, k * rows :],
                ],
                axis=1,
            )
        )
    packed = jnp.concatenate(packed, axis=0).reshape(ns, -1, full)
    payload = jnp.concatenate(
        [proj.reshape(2, ns, part, full).transpose(1, 0, 2, 3).reshape(ns, 2 * part, full), packed], axis=1
    )
    got = jnp.sum(a2a(payload, S).astype(F32), axis=0).astype(BF)
    got = a2a(jnp.broadcast_to(got[None], (ns,) + got.shape), S)
    h0 = got[:, :part].reshape(tok, full).astype(F32)
    e0 = got[:, part : 2 * part].reshape(tok, full).astype(F32)
    packed = got[:, 2 * part :].reshape(-1, full)

    def g_block(k, l):
        if k < ns // 2:
            return packed[k * rows : (k + 1) * rows, l * rows : (l + 1) * rows]
        m = ns - 1 - k
        at = (l - k - 1) * rows
        return packed[m * rows : (m + 1) * rows, at : at + rows]

    hs, acts, deltas = [], [], [None] * ns
    for l in range(ns):
        h = h0[:, l * rows : (l + 1) * rows]
        for k in range(l):
            h = h + mm(acts[k], g_block(k, l), ((1,), (0,)))
        hs.append(h)
        acts.append(jax.nn.silu(h).astype(BF))
    for l in reversed(range(ns)):
        e = e0[:, l * rows : (l + 1) * rows]
        for k in range(l + 1, ns):
            e = e + mm(deltas[k], g_block(l, k), ((1,), (1,)))
        deltas[l] = (e * silu_slope(hs[l])).astype(BF)
    act = jnp.concatenate(acts, axis=1)
    delta = jnp.concatenate(deltas, axis=1)

    cross = mm(act, delta, ((0,), (0,)))
    layer = jnp.arange(full) // rows
    upper = jnp.where(layer[:, None] < layer[None, :], cross, 0.0)
    cross_hi, cross_lo = split(upper + upper.T)
    grads = (
        mm(act, cotangent, ((0,), (0,)))
        + mm(delta, inputs, ((0,), (0,)))
        + mm(cross_hi, w, ((1,), (0,)))
        + mm(cross_lo, w, ((1,), (0,)))
    )
    grad = a2a(grads.astype(BF).reshape(ns, rows, cols), S).transpose(1, 0, 2).reshape(rows, width)

    table = dct_basis(64)
    fresh = DECAY * momentum[0, 0].astype(F32) + grad.astype(F32)
    blocks = fresh.reshape(rows, groups, 64)
    coef = jnp.einsum("kn,nbm,jm->bkj", table, blocks, table, precision=lax.Precision.HIGH)
    keep = keep_index[0, 0]
    lanes = jnp.arange(64, dtype=jnp.int32)
    row_hot = keep[:, :, None] // 64 == lanes
    col_hot = keep[:, :, None] % 64 == lanes
    mask = jnp.einsum("bik,bij->bkj", row_hot.astype(BF), col_hot.astype(BF), preferred_element_type=F32)
    picked = jnp.einsum("bik,bkj->bij", row_hot.astype(F32), coef, precision=lax.Precision.HIGH)
    values = jnp.sum(jnp.where(col_hot, picked, 0.0), axis=2)
    own_field = jnp.einsum("kn,bkj,jm->nbm", table, coef * mask, table, precision=lax.Precision.HIGH)
    momentum_out = (fresh - own_field.reshape(rows, width)).astype(BF)

    sent = jnp.concatenate([values.reshape(nd, -1), keep.astype(F32).reshape(nd, -1)], axis=1)
    seen = a2a(sent, DP)
    n = own * keep.shape[1]
    val = seen[:, :n].reshape(nd, own, -1).transpose(1, 0, 2).reshape(own, -1)
    pos = seen[:, n:].astype(jnp.int32).reshape(nd, own, -1).transpose(1, 0, 2).reshape(own, -1)
    val_hi, val_lo = split(val)
    row_hot = pos[:, :, None] // 64 == lanes
    col_hot = (pos[:, :, None] % 64 == lanes).astype(BF)
    summed = sum(
        jnp.einsum(
            "bik,bij->bkj", jnp.where(row_hot, v[:, :, None], 0).astype(BF), col_hot, preferred_element_type=F32
        )
        for v in (val_hi, val_lo)
    )
    decoded = jnp.einsum("kn,bkj,jm->nbm", table, summed, table, precision=lax.Precision.HIGH)
    decoded = decoded.reshape(64, own * 64).astype(BF)
    nc = nd // 2
    here = a2a(jnp.broadcast_to(decoded[None], (nc,) + decoded.shape), CHIP)
    there = swap_cores(here)
    update = jnp.stack([jnp.where(core == 0, here, there), jnp.where(core == 0, there, here)], axis=1)
    update = update.transpose(2, 0, 1, 3).reshape(rows, width)
    return (momentum_out[None, None], update[None, None])


def solution(mesh):
    fine = Mesh(mesh.devices.reshape(2, mesh.shape["section"] // 2, mesh.shape["dp"] // 16, 8, 2), ("zh", "x", "zl", "y", "core"))
    return jax.shard_map(
        local,
        mesh=fine,
        in_specs=(
            P(DP, S),
            P(DP, S),
            P(S, None, None),
            P(S, DP, None, None),
            P(S, DP, None, None),
        ),
        out_specs=(P(S, DP, None, None), P(S, DP, None, None)),
        check_vma=False,
    )
```

```python
import math

import jax
import jax.numpy as jnp
import numpy as np
from jax import lax
from jax.experimental import pallas as pl
from jax.experimental.pallas import tpu as pltpu
from jax.sharding import Mesh, PartitionSpec as P

DECAY = 0.999
S = ("zh", "x")
CHIP = ("zl", "y")
DP = ("zl", "y", "core")
F32 = jnp.float32
BF = jnp.bfloat16
LAYERS = 8


def a2a(value, axis):
    return lax.all_to_all(value, axis, 0, 0, tiled=True)


def swap_cores(value):
    return lax.ppermute(value, "core", [(0, 1), (1, 0)])


def mm(a, b):
    return lax.dot_general(a, b, (((1,), (0,)), ((), ())), preferred_element_type=F32)


def mm_nt(a, b):
    return lax.dot_general(a, b, (((1,), (1,)), ((), ())), preferred_element_type=F32)


def split(value):
    high = value.astype(BF)
    return high, (value - high.astype(F32)).astype(BF)


def dct_tables():
    n = np.arange(64)
    basis = np.cos(np.pi * (n[None, :] + 0.5) * n[:, None] / 64) * math.sqrt(2.0 / 64)
    basis[0] *= math.sqrt(0.5)
    return basis.astype(np.float32)


def pair(value):
    high = value.astype(jnp.bfloat16)
    low = (value - high.astype(np.float32)).astype(jnp.bfloat16)
    return high, low


def row_table(basis):
    high, low = pair(basis)
    return np.concatenate([high, high, low], axis=1)


def col_table(basis, count):
    high, low = pair(np.kron(np.eye(count, dtype=np.float32), basis))
    return np.concatenate([high, high, low], axis=0)


def by_rows(table, value):
    high, low = split(value)
    return mm(table, jnp.concatenate([high, low, high], axis=0))


def by_cols(value, table):
    high, low = split(value)
    return mm(jnp.concatenate([high, low, high], axis=1), table)


def whole(count):
    return [pl.BlockSpec(memory_space=pltpu.VMEM)] * count


SCALAR = pl.BlockSpec(memory_space=pltpu.SMEM)


def relay_kernel(core, got, x, g, mine, other, out, rhs):
    rows = 64
    at_mine = pl.multiple_of(core[0] * 32, 32)
    at_other = pl.multiple_of(32 - core[0] * 32, 32)
    for l in range(LAYERS):
        rhs[pl.ds(l * rows + at_mine, 32)] = mine[l]
        rhs[pl.ds(l * rows + at_other, 32)] = other[l]
    rhs[512:640] = g[...]
    rhs[640:768] = x[...]
    zero = jnp.zeros((rows, 128), BF)

    def block(l, p):
        if p < 2:
            return got[l, :, 256 + 128 * p : 384 + 128 * p]
        if l == 7:
            return got[0, :, 128 * p : 128 * p + 128]
        return got[7 - l, :, 384:512]

    acts, hs = [zero] * LAYERS, []
    for l in range(LAYERS):
        h = got[l, :, 0:128].astype(F32)
        pairs = range((l + 1) // 2)
        if len(pairs):
            left = jnp.concatenate([block(l, p) for p in pairs], axis=1)
            right = jnp.concatenate(acts[: 2 * len(pairs)], axis=0)
            h = h + mm(left, right)
        hs.append(h)
        acts[l] = (h * (1.0 / (1.0 + jnp.exp(-h)))).astype(BF)

    turned = {}
    for p in range(4):
        for q in range(p, 4):
            upper = zero if p == q else block(2 * q, p)
            both = jnp.concatenate([upper, block(2 * q + 1, p)], axis=0)
            turned[p, q] = both.T
    deltas = [zero] * LAYERS
    for l in reversed(range(LAYERS)):
        e = got[l, :, 128:256].astype(F32)
        pairs = range((l + 1) // 2, 4)
        if len(pairs):
            lo = rows * (l % 2)
            left = jnp.concatenate([turned[l // 2, q][lo : lo + rows] for q in pairs], axis=1)
            right = jnp.concatenate(deltas[2 * pairs[0] :], axis=0)
            e = e + mm(left, right)
        s = 1.0 / (1.0 + jnp.exp(-hs[l]))
        deltas[l] = (e * (s * (1.0 + hs[l] * (1.0 - s)))).astype(BF)

    act = jnp.concatenate(acts, axis=0)
    delta = jnp.concatenate(deltas, axis=0)
    row_layer = lax.broadcasted_iota(jnp.int32, (512, 512), 0) // rows
    col_layer = lax.broadcasted_iota(jnp.int32, (512, 512), 1) // rows
    cross = jnp.where(
        row_layer < col_layer, mm_nt(act, delta), jnp.where(row_layer > col_layer, mm_nt(delta, act), 0.0)
    ).astype(BF)
    lhs = jnp.concatenate([cross, act, delta], axis=1)
    for n in range(4):
        cols = slice(256 * n, 256 * n + 256)
        grads = mm(lhs, rhs[:, cols]).astype(BF)
        for l in range(LAYERS):
            out[l, :, cols] = grads[rows * l : rows * l + rows]


def coef_kernel(grad, momentum, keep, row_t, col_t, coef, sent):
    lane = lax.broadcasted_iota(jnp.int32, (1, 128), 1)
    sub = lax.broadcasted_iota(jnp.int32, (8, 128), 0)
    for s in range(8):
        fresh = DECAY * momentum[:, 1024 * s : 1024 * s + 1024].astype(F32) + grad[s].astype(F32)
        y = by_cols(jnp.concatenate([fresh[:, 256 * q : 256 * q + 256] for q in range(4)], axis=0), col_t[...])
        for q in range(4):
            z = by_rows(row_t[...], y[64 * q : 64 * q + 64])
            at = 1024 * s + 256 * q
            coef[:, at : at + 256] = z
            for u in range(2):
                t = 8 * s + 2 * q + u
                where = keep[t : t + 1, :]
                row = jnp.broadcast_to(where // 64, (8, 128))
                col = jnp.broadcast_to(where % 64 + (lane // 32) % 2 * 64, (8, 128))
                total = jnp.zeros((8, 128), F32)
                for r in range(8):
                    tile = z[8 * r : 8 * r + 8, 128 * u : 128 * u + 128]
                    picked = jnp.take_along_axis(tile, col, axis=1, mode="promise_in_bounds")
                    total = total + jnp.where(sub + 8 * r == row, picked, 0.0)
                value = jnp.sum(total, axis=0, keepdims=True)
                sent[t : t + 1, :] = jnp.where(lane < 64, value, where.astype(F32))


def rest_kernel(coef, keep, row_t, col_t, out):
    lane = lax.broadcasted_iota(jnp.int32, (1, 128), 1)
    row_id = lax.broadcasted_iota(jnp.int32, (64, 128), 0)
    col_id = lax.broadcasted_iota(jnp.int32, (128, 128), 0)
    for s in range(8):
        parts = []
        for q in range(4):
            halves = []
            for u in range(2):
                t = 8 * s + 2 * q + u
                where = keep[t : t + 1, :]
                row_hot = jnp.where((row_id == where // 64) & (lane < 64), 1.0, 0.0).astype(BF)
                col_hot = jnp.where(col_id == where % 64 + (lane // 32) % 2 * 64, 1.0, 0.0).astype(BF)
                kept = mm_nt(row_hot, col_hot)
                halves.append(jnp.where(kept > 0.5, 0.0, coef[:, 128 * t : 128 * t + 128]))
            parts.append(by_rows(row_t[...], jnp.concatenate(halves, axis=1)))
        y = by_cols(jnp.concatenate(parts, axis=0), col_t[...]).astype(BF)
        for q in range(4):
            at = 1024 * s + 256 * q
            out[:, at : at + 256] = y[64 * q : 64 * q + 64]


def owner_kernel(seen, row_t, col_t, out):
    lane = lax.broadcasted_iota(jnp.int32, (32, 128), 1)
    top, bottom = seen[0:32, :], seen[32:64, :]
    value = jnp.where(lane < 64, top, pltpu.roll(bottom, 64, 1))
    where = jnp.where(lane < 64, pltpu.roll(top, 64, 1), bottom).astype(jnp.int32)
    row = where // 64
    col = where % 64 + (lane // 32) % 2 * 64
    row_id = lax.broadcasted_iota(jnp.int32, (64, 128), 0)
    col_id = lax.broadcasted_iota(jnp.int32, (128, 128), 0)
    total = jnp.zeros((128, 128), F32)
    for t in range(0, 32, 2):
        lefts, rights = [], []
        for v in (t, t + 1):
            spread = jnp.where(row_id == row[v : v + 1, :], value[v : v + 1, :], 0.0)
            lefts.append(jnp.concatenate(split(spread), axis=0))
            rights.append(jnp.where(col_id == col[v : v + 1, :], 1.0, 0.0).astype(BF))
        total = total + mm_nt(jnp.concatenate(lefts, axis=1), jnp.concatenate(rights, axis=1))
    summed = total[0:64] + total[64:128]
    decoded = by_cols(by_rows(row_t[...], summed), col_t[...]).astype(BF)
    for m in range(out.shape[0]):
        out[m] = decoded


def join_kernel(core, here, there, out):
    def place(first, second):
        for m in range(32):
            out[:, 256 * m : 256 * m + 128] = first[m]
            out[:, 256 * m + 128 : 256 * m + 256] = second[m]

    @pl.when(core[0] == 0)
    def _():
        place(here, there)

    @pl.when(core[0] == 1)
    def _():
        place(there, here)


def call(kernel, name, out_shape, in_specs, args, scratch=(), flops=0):
    outs = jax.tree.map(lambda _: pl.BlockSpec(memory_space=pltpu.VMEM), out_shape)
    return pl.pallas_call(
        kernel,
        out_shape=out_shape,
        in_specs=in_specs,
        out_specs=outs,
        scratch_shapes=list(scratch),
        name=name,
        compiler_params=pltpu.CompilerParams(vmem_limit_bytes=32 * 1024 * 1024),
        cost_estimate=pl.CostEstimate(flops=flops, bytes_accessed=0, transcendentals=0),
    )(*args)


def local(inputs, cotangent, weights, momentum, keep_index):
    core = lax.axis_index("core").astype(jnp.int32)
    core_at = core.reshape(1)
    weight = weights[0]
    rows, width = weight.shape
    cols = width // LAYERS
    full = LAYERS * rows
    struct = jax.ShapeDtypeStruct

    half = lax.dynamic_slice_in_dim(weight, core * (rows // 2), rows // 2, 0)
    mine = a2a(half.reshape(rows // 2, LAYERS, cols).transpose(1, 0, 2), S)
    other = swap_cores(mine)
    w = jnp.concatenate(
        [jnp.where(core == 0, mine, other), jnp.where(core == 0, other, mine)], axis=1
    ).reshape(full, cols)

    proj = mm_nt(w, jnp.concatenate([inputs, cotangent], axis=0)).astype(BF).reshape(LAYERS, rows, 256)
    gram = mm_nt(w, w).astype(BF).reshape(LAYERS, rows, full)
    packed = jnp.stack(
        [gram[7, :, 256:]]
        + [jnp.concatenate([gram[l, :, :128], gram[7 - l, :, 256:384]], axis=1) for l in (1, 2)]
        + [gram[l, :, :256] for l in range(3, LAYERS)]
    )
    payload = jnp.concatenate([proj, packed], axis=2)
    got = jnp.sum(a2a(payload, S).astype(F32), axis=0).astype(BF)
    got = a2a(jnp.broadcast_to(got[None], (LAYERS,) + got.shape), S)

    grads = call(
        relay_kernel,
        "relay",
        struct((LAYERS, rows, cols), BF),
        [SCALAR] + whole(5),
        (core_at, got, inputs, cotangent, mine, other),
        [pltpu.VMEM((768, cols), BF)],
        2 * 512 * 768 * 1024,
    )
    grad = a2a(grads, S)

    basis = dct_tables()
    keep = keep_index[0, 0].reshape(64, 64)
    keep = jnp.concatenate([keep, keep], axis=1)
    coef, sent = call(
        coef_kernel,
        "coef",
        (struct((rows, width), F32), struct((64, 128), F32)),
        whole(5),
        (grad, momentum[0, 0], keep, row_table(basis), col_table(basis.T, 4)),
        (),
        2 * 2048 * 768 * 256,
    )
    seen = a2a(sent, DP)
    momentum_out = call(
        rest_kernel,
        "rest",
        struct((rows, width), BF),
        whole(4),
        (coef, keep, row_table(basis.T), col_table(basis, 4)),
        (),
        2 * 2048 * 768 * 256 * 4,
    )

    spread = call(
        owner_kernel,
        "owner",
        struct((32, 64, 128), BF),
        whole(3),
        (seen, row_table(basis.T), col_table(basis, 2)),
        (),
        2 * 64 * 128 * 4096,
    )
    here = a2a(spread, CHIP)
    there = swap_cores(here)
    update = call(
        join_kernel, "join", struct((rows, width), BF), [SCALAR] + whole(2), (core_at, here, there), (), 1000
    )
    return (momentum_out[None, None], update[None, None])


def solution(mesh):
    fine = Mesh(mesh.devices.reshape(2, 4, 4, 8, 2), ("zh", "x", "zl", "y", "core"))
    return jax.shard_map(
        local,
        mesh=fine,
        in_specs=(
            P(DP, S),
            P(DP, S),
            P(S, None, None),
            P(S, DP, None, None),
            P(S, DP, None, None),
        ),
        out_specs=(P(S, DP, None, None), P(S, DP, None, None)),
        check_vma=False,
    )
```

```python
import math

import jax
import jax.numpy as jnp
import numpy as np
from jax import lax
from jax.experimental import pallas as pl
from jax.experimental.pallas import tpu as pltpu
from jax.sharding import Mesh, PartitionSpec as P


DECAY = 0.999
S = ("zh", "x")
CHIP = ("zl", "y")
DP = ("zl", "y", "core")
F32 = jnp.float32
BF = jnp.bfloat16
LAYERS = 8


def a2a(value, axis):
    return lax.all_to_all(value, axis, 0, 0, tiled=True)


def swap_cores(value):
    return lax.ppermute(value, "core", [(0, 1), (1, 0)])


def mm(a, b):
    return lax.dot_general(a, b, (((1,), (0,)), ((), ())), preferred_element_type=F32)


def mm_nt(a, b):
    return lax.dot_general(a, b, (((1,), (1,)), ((), ())), preferred_element_type=F32)


def split(value):
    high = value.astype(BF)
    return high, (value - high.astype(F32)).astype(BF)


def dct_tables():
    n = np.arange(64)
    basis = np.cos(np.pi * (n[None, :] + 0.5) * n[:, None] / 64) * math.sqrt(2.0 / 64)
    basis[0] *= math.sqrt(0.5)
    return basis.astype(np.float32)


def pair(value):
    high = value.astype(jnp.bfloat16)
    low = (value - high.astype(np.float32)).astype(jnp.bfloat16)
    return high, low


def row_table(basis):
    high, low = pair(basis)
    return np.concatenate([high, high, low], axis=1)


def col_table(basis, count):
    high, low = pair(np.kron(np.eye(count, dtype=np.float32), basis))
    return np.concatenate([high, high, low], axis=0)


def by_rows(table, value):
    high, low = split(value)
    return mm(table, jnp.concatenate([high, low, high], axis=0))


def by_cols(value, table):
    high, low = split(value)
    return mm(jnp.concatenate([high, low, high], axis=1), table)


def whole(count):
    return [pl.BlockSpec(memory_space=pltpu.VMEM)] * count


SCALAR = pl.BlockSpec(memory_space=pltpu.SMEM)


def relay_kernel(core, got, x, g, mine, other, out, rhs):
    rows = 64
    at_mine = pl.multiple_of(core[0] * 32, 32)
    at_other = pl.multiple_of(32 - core[0] * 32, 32)
    for l in range(LAYERS):
        rhs[pl.ds(l * rows + at_mine, 32)] = mine[l]
        rhs[pl.ds(l * rows + at_other, 32)] = other[l]
    rhs[512:640] = g[...]
    rhs[640:768] = x[...]
    zero = jnp.zeros((rows, 128), BF)

    def block(l, p):
        if p < 2:
            return got[l % 4, l // 4, :, 256 + 128 * p : 384 + 128 * p]
        if l == 7:
            return got[0, 0, :, 128 * p : 128 * p + 128]
        return got[7 - l, 0, :, 384:512]

    acts, hs = [zero] * LAYERS, []
    for l in range(LAYERS):
        h = got[l % 4, l // 4, :, 0:128].astype(F32)
        pairs = range((l + 1) // 2)
        if len(pairs):
            left = jnp.concatenate([block(l, p) for p in pairs], axis=1)
            right = jnp.concatenate(acts[: 2 * len(pairs)], axis=0)
            h = h + mm(left, right)
        hs.append(h)
        acts[l] = (h * (1.0 / (1.0 + jnp.exp(-h)))).astype(BF)

    turned = {}
    for p in range(4):
        for q in range(p, 4):
            upper = zero if p == q else block(2 * q, p)
            both = jnp.concatenate([upper, block(2 * q + 1, p)], axis=0)
            turned[p, q] = both.T
    deltas = [zero] * LAYERS
    for l in reversed(range(LAYERS)):
        e = got[l % 4, l // 4, :, 128:256].astype(F32)
        pairs = range((l + 1) // 2, 4)
        if len(pairs):
            lo = rows * (l % 2)
            left = jnp.concatenate([turned[l // 2, q][lo : lo + rows] for q in pairs], axis=1)
            right = jnp.concatenate(deltas[2 * pairs[0] :], axis=0)
            e = e + mm(left, right)
        s = 1.0 / (1.0 + jnp.exp(-hs[l]))
        deltas[l] = (e * (s * (1.0 + hs[l] * (1.0 - s)))).astype(BF)

    act = jnp.concatenate(acts, axis=0)
    delta = jnp.concatenate(deltas, axis=0)
    row_layer = lax.broadcasted_iota(jnp.int32, (512, 512), 0) // rows
    col_layer = lax.broadcasted_iota(jnp.int32, (512, 512), 1) // rows
    cross = jnp.where(
        row_layer < col_layer, mm_nt(act, delta), jnp.where(row_layer > col_layer, mm_nt(delta, act), 0.0)
    ).astype(BF)
    lhs = jnp.concatenate([cross, act, delta], axis=1)
    for n in range(4):
        cols = slice(256 * n, 256 * n + 256)
        grads = mm(lhs, rhs[:, cols]).astype(BF)
        for l in range(LAYERS):
            out[l, :, cols] = grads[rows * l : rows * l + rows]


def pick(z, row, col, lane):
    sub = lax.broadcasted_iota(jnp.int32, (8, 128), 0)
    row = jnp.broadcast_to(row, (8, 128))
    col = jnp.broadcast_to(col + (lane // 32) % 2 * 64, (8, 128))
    first = jnp.broadcast_to(lane < 64, (8, 128))
    total = jnp.zeros((8, 128), F32)
    for r in range(8):
        left, right = (
            jnp.take_along_axis(
                z[8 * r : 8 * r + 8, 128 * u : 128 * u + 128], col, axis=1, mode="promise_in_bounds"
            )
            for u in range(2)
        )
        total = total + jnp.where(sub + 8 * r == row, jnp.where(first, left, right), 0.0)
    return jnp.sum(total, axis=0, keepdims=True)


def choose(field, keep, row_t, col_t, vals):
    lane = lax.broadcasted_iota(jnp.int32, (1, 128), 1)
    for s in range(8):
        piece = field(s)
        y = by_cols(jnp.concatenate([piece[:, 256 * q : 256 * q + 256] for q in range(4)], axis=0), col_t[...])
        for q in range(4):
            t = 4 * s + q
            z = by_rows(row_t[...], y[64 * q : 64 * q + 64])
            where = keep[t : t + 1, :]
            vals[t : t + 1, :] = pick(z, where // 64, where % 64, lane)


def past_kernel(momentum, keep, row_t, col_t, vals):
    choose(lambda s: DECAY * momentum[:, 1024 * s : 1024 * s + 1024].astype(F32), keep, row_t, col_t, vals)


def coef_kernel(grad, past, keep, row_t, col_t, vals, sent):
    choose(lambda s: grad[s].astype(F32), keep, row_t, col_t, vals)
    value = vals[...] + past[...]
    vals[...] = value
    where = keep[...].astype(F32)
    first = lax.broadcasted_iota(jnp.int32, (32, 128), 1) < 64
    sent[0:32, :] = jnp.where(first, value, pltpu.roll(where, 64, 1))
    sent[32:64, :] = jnp.where(first, pltpu.roll(value, 64, 1), where)


def half_kernel(core, weight, out, sems):
    at = pl.multiple_of(core[0] * 32, 32)
    copies = [
        pltpu.make_async_copy(weight.at[pl.ds(at, 32), pl.ds(1024 * s, 1024)], out.at[s], sems.at[s])
        for s in range(LAYERS)
    ]
    for copy in copies:
        copy.start()
    for copy in copies:
        copy.wait()


def rest_kernel(vals, keep, momentum, grad, row_t, col_t, out):
    lane = lax.broadcasted_iota(jnp.int32, (1, 128), 1)
    row_id = lax.broadcasted_iota(jnp.int32, (64, 128), 0)
    col_id = lax.broadcasted_iota(jnp.int32, (256, 128), 0)
    for s in range(8):
        parts = []
        for q in range(4):
            t = 4 * s + q
            where = keep[t : t + 1, :]
            spread = jnp.where(row_id == where // 64, vals[t : t + 1, :], 0.0)
            col_hot = jnp.where(col_id == where % 64 + lane // 32 * 64, 1.0, 0.0).astype(BF)
            both = mm_nt(jnp.concatenate(split(spread), axis=0), col_hot)
            parts.append(by_rows(row_t[...], both[0:64] + both[64:128]))
        y = by_cols(jnp.concatenate(parts, axis=0), col_t[...])
        for q in range(4):
            at = 256 * q
            cols = slice(1024 * s + at, 1024 * s + at + 256)
            fresh = DECAY * momentum[:, cols].astype(F32) + grad[s, :, at : at + 256].astype(F32)
            out[:, cols] = (fresh - y[64 * q : 64 * q + 64]).astype(BF)


def owner_kernel(seen, row_t, col_t, out):
    lane = lax.broadcasted_iota(jnp.int32, (32, 128), 1)
    top, bottom = seen[0:32, :], seen[32:64, :]
    value = jnp.where(lane < 64, top, pltpu.roll(bottom, 64, 1))
    where = jnp.where(lane < 64, pltpu.roll(top, 64, 1), bottom).astype(jnp.int32)
    row = where // 64
    col = where % 64 + (lane // 32) % 2 * 64
    row_id = lax.broadcasted_iota(jnp.int32, (64, 128), 0)
    col_id = lax.broadcasted_iota(jnp.int32, (128, 128), 0)
    total = jnp.zeros((128, 128), F32)
    for t in range(0, 32, 2):
        lefts, rights = [], []
        for v in (t, t + 1):
            spread = jnp.where(row_id == row[v : v + 1, :], value[v : v + 1, :], 0.0)
            lefts.append(jnp.concatenate(split(spread), axis=0))
            rights.append(jnp.where(col_id == col[v : v + 1, :], 1.0, 0.0).astype(BF))
        total = total + mm_nt(jnp.concatenate(lefts, axis=1), jnp.concatenate(rights, axis=1))
    summed = total[0:64] + total[64:128]
    decoded = by_cols(by_rows(row_t[...], summed), col_t[...]).astype(BF)
    for m in range(out.shape[0]):
        out[m] = decoded


def join_kernel(core, here, there, out):
    def place(first, second):
        for m in range(32):
            for owner, blocks in ((2 * m, first), (2 * m + 1, second)):
                at = 256 * (owner % 32) + 128 * (owner // 32)
                out[:, at : at + 128] = blocks[m]

    @pl.when(core[0] == 0)
    def _():
        place(here, there)

    @pl.when(core[0] == 1)
    def _():
        place(there, here)


def call(kernel, out_shape, in_specs, args, scratch=(), flops=0):
    outs = jax.tree.map(lambda _: pl.BlockSpec(memory_space=pltpu.VMEM), out_shape)
    return pl.pallas_call(
        kernel,
        out_shape=out_shape,
        in_specs=in_specs,
        out_specs=outs,
        scratch_shapes=list(scratch),
        compiler_params=pltpu.CompilerParams(vmem_limit_bytes=32 * 1024 * 1024),
        cost_estimate=pl.CostEstimate(flops=flops, bytes_accessed=0, transcendentals=0),
    )(*args)


def step(inputs, cotangent, weights, momentum, keep_index):
    core = lax.axis_index("core").astype(jnp.int32)
    core_at = core.reshape(1)
    weight = weights[0]
    rows, width = weight.shape
    cols = width // LAYERS
    full = LAYERS * rows
    struct = jax.ShapeDtypeStruct

    half = call(
        half_kernel,
        struct((LAYERS, rows // 2, cols), BF),
        [SCALAR, pl.BlockSpec(memory_space=pltpu.HBM)],
        (core_at, weight),
        [pltpu.SemaphoreType.DMA((LAYERS,))],
        1000,
    )
    mine = a2a(half, S)
    other = swap_cores(mine)
    w = jnp.concatenate(
        [jnp.where(core == 0, mine, other), jnp.where(core == 0, other, mine)], axis=1
    ).reshape(full, cols)

    proj = mm_nt(w, jnp.concatenate([inputs, cotangent], axis=0)).astype(BF).reshape(LAYERS, rows, 256)
    gram = mm_nt(w, w).astype(BF).reshape(LAYERS, rows, full)
    packed = (
        [gram[7, :, 256:]]
        + [jnp.concatenate([gram[l, :, :128], gram[7 - l, :, 256:384]], axis=1) for l in (1, 2)]
        + [gram[l, :, :256] for l in range(3, LAYERS)]
    )
    chunks = [jnp.concatenate([proj[l], packed[l]], axis=1) for l in range(LAYERS)]
    payload = jnp.stack([jnp.stack([chunks[x], chunks[x + 4]]) for x in range(4)])
    part = jnp.sum(a2a(payload, "x").astype(F32), axis=0).astype(BF)
    far = lax.ppermute(part, "zh", [(0, 1), (1, 0)])
    got = (part.astype(F32) + far.astype(F32)).astype(BF)
    got = a2a(jnp.broadcast_to(got[None], (4,) + got.shape), "x")

    grads = call(
        relay_kernel,
        struct((LAYERS, rows, cols), BF),
        [SCALAR] + whole(5),
        (core_at, got, inputs, cotangent, mine, other),
        [pltpu.VMEM((768, cols), BF)],
        2 * 512 * 768 * 1024,
    )
    grad = a2a(grads, S)

    basis = dct_tables()
    keep = keep_index[0, 0].reshape(32, 128)
    values = struct((32, 128), F32)
    tables = (row_table(basis), col_table(basis.T, 4))
    flops = 2 * 2048 * 768 * 256
    past = call(past_kernel, values, whole(4), (momentum[0, 0], keep) + tables, (), flops)
    vals, sent = call(coef_kernel, (values, struct((64, 128), F32)), whole(5), (grad, past, keep) + tables, (), flops)
    seen = a2a(sent, DP)
    momentum_out = call(
        rest_kernel,
        struct((rows, width), BF),
        whole(6),
        (vals, keep, momentum[0, 0], grad, row_table(basis.T), col_table(basis, 4)),
        (),
        2 * 2048 * 768 * 256 * 4,
    )

    spread = call(
        owner_kernel,
        struct((32, 64, 128), BF),
        whole(3),
        (seen, row_table(basis.T), col_table(basis, 2)),
        (),
        2 * 64 * 128 * 4096,
    )
    here = a2a(spread, CHIP)
    there = swap_cores(here)
    update = call(join_kernel, struct((rows, width), BF), [SCALAR] + whole(2), (core_at, here, there), (), 1000)
    return (momentum_out[None, None], update[None, None])


def solution(mesh):
    fine = Mesh(mesh.devices.reshape(2, 4, 4, 8, 2), ("zh", "x", "zl", "y", "core"))
    return jax.shard_map(
        step,
        mesh=fine,
        in_specs=(
            P(DP, S),
            P(DP, S),
            P(S, None, None),
            P(S, DP, None, None),
            P(S, DP, None, None),
        ),
        out_specs=(P(S, DP, None, None), P(S, DP, None, None)),
        check_vma=False,
    )
```

```python
import math

import jax
import jax.numpy as jnp
import numpy as np
from jax import lax
from jax.experimental import pallas as pl
from jax.experimental.pallas import tpu as pltpu
from jax.sharding import Mesh, PartitionSpec as P


DECAY = 0.999
S = ("zh", "x")
CHIP = ("zl", "y")
DP = ("zl", "y", "core")
F32 = jnp.float32
BF = jnp.bfloat16
LAYERS = 8


def a2a(value, axis):
    return lax.all_to_all(value, axis, 0, 0, tiled=True)


def swap_cores(value):
    return lax.ppermute(value, "core", [(0, 1), (1, 0)])


def mm(a, b):
    return lax.dot_general(a, b, (((1,), (0,)), ((), ())), preferred_element_type=F32)


def mm_nt(a, b):
    return lax.dot_general(a, b, (((1,), (1,)), ((), ())), preferred_element_type=F32)


def split(value):
    high = value.astype(BF)
    return high, (value - high.astype(F32)).astype(BF)


def dct_tables():
    n = np.arange(64)
    basis = np.cos(np.pi * (n[None, :] + 0.5) * n[:, None] / 64) * math.sqrt(2.0 / 64)
    basis[0] *= math.sqrt(0.5)
    return basis.astype(np.float32)


def pair(value):
    high = value.astype(jnp.bfloat16)
    low = (value - high.astype(np.float32)).astype(jnp.bfloat16)
    return high, low


def row_table(basis):
    high, low = pair(basis)
    return np.concatenate([high, high, low], axis=1)


def col_table(basis, count):
    high, low = pair(np.kron(np.eye(count, dtype=np.float32), basis))
    return np.concatenate([high, high, low], axis=0)


def by_rows(table, value):
    high, low = split(value)
    return mm(table, jnp.concatenate([high, low, high], axis=0))


def by_cols(value, table):
    high, low = split(value)
    return mm(jnp.concatenate([high, low, high], axis=1), table)


def whole(count):
    return [pl.BlockSpec(memory_space=pltpu.VMEM)] * count


SCALAR = pl.BlockSpec(memory_space=pltpu.SMEM)


def relay_kernel(core, got, x, g, mine, other, out, rhs):
    rows = 64
    at_mine = pl.multiple_of(core[0] * 32, 32)
    at_other = pl.multiple_of(32 - core[0] * 32, 32)
    for l in range(LAYERS):
        rhs[l * rows : l * rows + 32] = mine[l]
        rhs[l * rows + 32 : l * rows + 64] = other[l]
    rhs[512:640] = g[...]
    rhs[640:768] = x[...]
    zero = jnp.zeros((rows, 128), BF)

    def block(l, p):
        if p < 2:
            return got[l % 4, l // 4, :, 256 + 128 * p : 384 + 128 * p]
        if l == 7:
            return got[0, 0, :, 128 * p : 128 * p + 128]
        return got[7 - l, 0, :, 384:512]

    acts, hs = [zero] * LAYERS, []
    for l in range(LAYERS):
        h = got[l % 4, l // 4, :, 0:128].astype(F32)
        pairs = range((l + 1) // 2)
        if len(pairs):
            left = jnp.concatenate([block(l, p) for p in pairs], axis=1)
            right = jnp.concatenate(acts[: 2 * len(pairs)], axis=0)
            h = h + mm(left, right)
        hs.append(h)
        acts[l] = (h * (1.0 / (1.0 + jnp.exp(-h)))).astype(BF)

    turned = {}
    for p in range(4):
        for q in range(p, 4):
            upper = zero if p == q else block(2 * q, p)
            both = jnp.concatenate([upper, block(2 * q + 1, p)], axis=0)
            turned[p, q] = both.T
    deltas = [zero] * LAYERS
    for l in reversed(range(LAYERS)):
        e = got[l % 4, l // 4, :, 128:256].astype(F32)
        pairs = range((l + 1) // 2, 4)
        if len(pairs):
            lo = rows * (l % 2)
            left = jnp.concatenate([turned[l // 2, q][lo : lo + rows] for q in pairs], axis=1)
            right = jnp.concatenate(deltas[2 * pairs[0] :], axis=0)
            e = e + mm(left, right)
        s = 1.0 / (1.0 + jnp.exp(-hs[l]))
        deltas[l] = (e * (s * (1.0 + hs[l] * (1.0 - s)))).astype(BF)

    act = jnp.concatenate(acts, axis=0)
    delta = jnp.concatenate(deltas, axis=0)
    row_layer = lax.broadcasted_iota(jnp.int32, (512, 512), 0) // rows
    col_layer = lax.broadcasted_iota(jnp.int32, (512, 512), 1) // rows
    cross = jnp.where(
        row_layer < col_layer, mm_nt(act, delta), jnp.where(row_layer > col_layer, mm_nt(delta, act), 0.0)
    ).astype(BF)
    lhs = jnp.concatenate([cross, act, delta], axis=1)
    for n in range(4):
        cols = slice(256 * n, 256 * n + 256)
        grads = mm(lhs, rhs[:, cols]).astype(BF)
        for l in range(LAYERS):
            out[l, pl.ds(at_mine, 32), cols] = grads[rows * l : rows * l + 32]
            out[l, pl.ds(at_other, 32), cols] = grads[rows * l + 32 : rows * l + 64]


def pick(z, row, col, lane):
    sub = lax.broadcasted_iota(jnp.int32, (8, 128), 0)
    row = jnp.broadcast_to(row, (8, 128))
    col = jnp.broadcast_to(col + (lane // 32) % 2 * 64, (8, 128))
    first = jnp.broadcast_to(lane < 64, (8, 128))
    total = jnp.zeros((8, 128), F32)
    for r in range(8):
        left, right = (
            jnp.take_along_axis(
                z[8 * r : 8 * r + 8, 128 * u : 128 * u + 128], col, axis=1, mode="promise_in_bounds"
            )
            for u in range(2)
        )
        total = total + jnp.where(sub + 8 * r == row, jnp.where(first, left, right), 0.0)
    return jnp.sum(total, axis=0, keepdims=True)


def choose(field, keep, row_t, col_t, vals):
    lane = lax.broadcasted_iota(jnp.int32, (1, 128), 1)
    for s in range(8):
        piece = field(s)
        piece = jnp.concatenate([piece[:, 256 * q : 256 * q + 256] for q in range(4)], axis=0)
        if piece.dtype == BF:
            y = mm(jnp.concatenate([piece, piece], axis=1), col_t[256:768])
        else:
            y = by_cols(piece, col_t[...])
        for q in range(4):
            t = 4 * s + q
            z = by_rows(row_t[...], y[64 * q : 64 * q + 64])
            where = keep[t : t + 1, :]
            vals[t : t + 1, :] = pick(z, where // 64, where % 64, lane)


def past_kernel(momentum, keep, row_t, col_t, vals):
    choose(lambda s: DECAY * momentum[:, 1024 * s : 1024 * s + 1024].astype(F32), keep, row_t, col_t, vals)


def coef_kernel(grad, past, keep, row_t, col_t, vals, sent):
    choose(lambda s: grad[s], keep, row_t, col_t, vals)
    value = vals[...] + past[...]
    vals[...] = value
    where = keep[...].astype(F32)
    first = lax.broadcasted_iota(jnp.int32, (32, 128), 1) < 64
    sent[0:32, :] = jnp.where(first, value, pltpu.roll(where, 64, 1))
    sent[32:64, :] = jnp.where(first, pltpu.roll(value, 64, 1), where)


def half_kernel(core, weight, out, sems):
    at = pl.multiple_of(core[0] * 32, 32)
    copies = [
        pltpu.make_async_copy(weight.at[pl.ds(at, 32), pl.ds(1024 * s, 1024)], out.at[s], sems.at[s])
        for s in range(LAYERS)
    ]
    for copy in copies:
        copy.start()
    for copy in copies:
        copy.wait()


def rest_kernel(vals, keep, momentum, grad, row_t, col_t, out):
    lane = lax.broadcasted_iota(jnp.int32, (1, 128), 1)
    row_id = lax.broadcasted_iota(jnp.int32, (64, 128), 0)
    col_id = lax.broadcasted_iota(jnp.int32, (256, 128), 0)
    for s in range(8):
        parts = []
        for q in range(4):
            t = 4 * s + q
            where = keep[t : t + 1, :]
            spread = jnp.where(row_id == where // 64, vals[t : t + 1, :], 0.0)
            col_hot = jnp.where(col_id == where % 64 + lane // 32 * 64, 1.0, 0.0).astype(BF)
            both = mm_nt(jnp.concatenate(split(spread), axis=0), col_hot)
            parts.append(by_rows(row_t[...], both[0:64] + both[64:128]))
        y = by_cols(jnp.concatenate(parts, axis=0), col_t[...])
        for q in range(4):
            at = 256 * q
            cols = slice(1024 * s + at, 1024 * s + at + 256)
            fresh = DECAY * momentum[:, cols].astype(F32) + grad[s, :, at : at + 256].astype(F32)
            out[:, cols] = (fresh - y[64 * q : 64 * q + 64]).astype(BF)


def owner_kernel(seen, row_t, col_t, out):
    lane = lax.broadcasted_iota(jnp.int32, (32, 128), 1)
    top, bottom = seen[0:32, :], seen[32:64, :]
    value = jnp.where(lane < 64, top, pltpu.roll(bottom, 64, 1))
    where = jnp.where(lane < 64, pltpu.roll(top, 64, 1), bottom).astype(jnp.int32)
    row = where // 64
    col = where % 64 + (lane // 32) % 2 * 64
    row_id = lax.broadcasted_iota(jnp.int32, (64, 128), 0)
    col_id = lax.broadcasted_iota(jnp.int32, (128, 128), 0)
    total = jnp.zeros((128, 128), F32)
    for t in range(0, 32, 2):
        lefts, rights = [], []
        for v in (t, t + 1):
            spread = jnp.where(row_id == row[v : v + 1, :], value[v : v + 1, :], 0.0)
            lefts.append(jnp.concatenate(split(spread), axis=0))
            rights.append(jnp.where(col_id == col[v : v + 1, :], 1.0, 0.0).astype(BF))
        total = total + mm_nt(jnp.concatenate(lefts, axis=1), jnp.concatenate(rights, axis=1))
    summed = total[0:64] + total[64:128]
    decoded = by_cols(by_rows(row_t[...], summed), col_t[...]).astype(BF)
    for m in range(out.shape[0]):
        out[m] = decoded


def join_kernel(core, here, there, out):
    def place(first, second):
        for m in range(32):
            for owner, blocks in ((2 * m, first), (2 * m + 1, second)):
                at = 256 * (owner % 32) + 128 * (owner // 32)
                out[:, at : at + 128] = blocks[m]

    @pl.when(core[0] == 0)
    def _():
        place(here, there)

    @pl.when(core[0] == 1)
    def _():
        place(there, here)


def call(kernel, out_shape, in_specs, args, scratch=(), flops=0):
    outs = jax.tree.map(lambda _: pl.BlockSpec(memory_space=pltpu.VMEM), out_shape)
    return pl.pallas_call(
        kernel,
        out_shape=out_shape,
        in_specs=in_specs,
        out_specs=outs,
        scratch_shapes=list(scratch),
        compiler_params=pltpu.CompilerParams(vmem_limit_bytes=32 * 1024 * 1024),
        cost_estimate=pl.CostEstimate(flops=flops, bytes_accessed=0, transcendentals=0),
    )(*args)


def step(inputs, cotangent, weights, momentum, keep_index):
    core = lax.axis_index("core").astype(jnp.int32)
    core_at = core.reshape(1)
    weight = weights[0]
    rows, width = weight.shape
    cols = width // LAYERS
    full = LAYERS * rows
    struct = jax.ShapeDtypeStruct

    half = call(
        half_kernel,
        struct((LAYERS, rows // 2, cols), BF),
        [SCALAR, pl.BlockSpec(memory_space=pltpu.HBM)],
        (core_at, weight),
        [pltpu.SemaphoreType.DMA((LAYERS,))],
        1000,
    )
    mine = a2a(half, S)
    other = swap_cores(mine)
    w = jnp.concatenate([mine, other], axis=1).reshape(full, cols)

    proj = mm_nt(w, jnp.concatenate([inputs, cotangent], axis=0)).astype(BF).reshape(LAYERS, rows, 256)
    gram = mm_nt(w, w).astype(BF).reshape(LAYERS, rows, full)
    packed = (
        [gram[7, :, 256:]]
        + [jnp.concatenate([gram[l, :, :128], gram[7 - l, :, 256:384]], axis=1) for l in (1, 2)]
        + [gram[l, :, :256] for l in range(3, LAYERS)]
    )
    chunks = [jnp.concatenate([proj[l], packed[l]], axis=1) for l in range(LAYERS)]
    payload = jnp.stack([jnp.stack([chunks[x], chunks[x + 4]]) for x in range(4)])
    part = jnp.sum(a2a(payload, "x").astype(F32), axis=0).astype(BF)
    far = lax.ppermute(part, "zh", [(0, 1), (1, 0)])
    got = (part.astype(F32) + far.astype(F32)).astype(BF)
    got = a2a(jnp.broadcast_to(got[None], (4,) + got.shape), "x")

    grads = call(
        relay_kernel,
        struct((LAYERS, rows, cols), BF),
        [SCALAR] + whole(5),
        (core_at, got, inputs, cotangent, mine, other),
        [pltpu.VMEM((768, cols), BF)],
        2 * 512 * 768 * 1024,
    )
    grad = a2a(grads, S)

    basis = dct_tables()
    keep = keep_index[0, 0].reshape(32, 128)
    values = struct((32, 128), F32)
    tables = (row_table(basis), col_table(basis.T, 4))
    flops = 2 * 2048 * 768 * 256
    past = call(past_kernel, values, whole(4), (momentum[0, 0], keep) + tables, (), flops)
    vals, sent = call(coef_kernel, (values, struct((64, 128), F32)), whole(5), (grad, past, keep) + tables, (), flops)
    seen = a2a(sent, DP)
    momentum_out = call(
        rest_kernel,
        struct((rows, width), BF),
        whole(6),
        (vals, keep, momentum[0, 0], grad, row_table(basis.T), col_table(basis, 4)),
        (),
        2 * 2048 * 768 * 256 * 4,
    )

    spread = call(
        owner_kernel,
        struct((32, 64, 128), BF),
        whole(3),
        (seen, row_table(basis.T), col_table(basis, 2)),
        (),
        2 * 64 * 128 * 4096,
    )
    here = a2a(spread, CHIP)
    there = swap_cores(here)
    update = call(join_kernel, struct((rows, width), BF), [SCALAR] + whole(2), (core_at, here, there), (), 1000)
    return (momentum_out[None, None], update[None, None])


def solution(mesh):
    fine = Mesh(mesh.devices.reshape(2, 4, 4, 8, 2), ("zh", "x", "zl", "y", "core"))
    return jax.shard_map(
        step,
        mesh=fine,
        in_specs=(
            P(DP, S),
            P(DP, S),
            P(S, None, None),
            P(S, DP, None, None),
            P(S, DP, None, None),
        ),
        out_specs=(P(S, DP, None, None), P(S, DP, None, None)),
        check_vma=False,
    )
```

```python
import math

import jax
import jax.numpy as jnp
import numpy as np
from jax import lax
from jax.experimental import pallas as pl
from jax.experimental.pallas import tpu as pltpu
from jax.sharding import Mesh, PartitionSpec as P


DECAY = 0.999
S = ("zh", "x")
CHIP = ("zl", "y")
DP = ("zl", "y", "core")
F32 = jnp.float32
BF = jnp.bfloat16
LAYERS = 8


def a2a(value, axis):
    return lax.all_to_all(value, axis, 0, 0, tiled=True)


def swap_cores(value):
    return lax.ppermute(value, "core", [(0, 1), (1, 0)])


def mm(a, b):
    return lax.dot_general(a, b, (((1,), (0,)), ((), ())), preferred_element_type=F32)


def mm_nt(a, b):
    return lax.dot_general(a, b, (((1,), (1,)), ((), ())), preferred_element_type=F32)


def split(value):
    high = value.astype(BF)
    return high, (value - high.astype(F32)).astype(BF)


def dct_tables():
    n = np.arange(64)
    basis = np.cos(np.pi * (n[None, :] + 0.5) * n[:, None] / 64) * math.sqrt(2.0 / 64)
    basis[0] *= math.sqrt(0.5)
    return basis.astype(np.float32)


def pair(value):
    high = value.astype(jnp.bfloat16)
    low = (value - high.astype(np.float32)).astype(jnp.bfloat16)
    return high, low


def row_table(basis):
    high, low = pair(basis)
    return np.concatenate([high, high, low], axis=1)


def col_table(basis, count):
    high, low = pair(np.kron(np.eye(count, dtype=np.float32), basis))
    return np.concatenate([high, high, low], axis=0)


def by_rows(table, value):
    high, low = split(value)
    return mm(table, jnp.concatenate([high, low, high], axis=0))


def by_cols(value, table):
    high, low = split(value)
    return mm(jnp.concatenate([high, low, high], axis=1), table)


def whole(count):
    return [pl.BlockSpec(memory_space=pltpu.VMEM)] * count


SCALAR = pl.BlockSpec(memory_space=pltpu.SMEM)


def relay_kernel(core, got, x, g, mine, other, out, rhs):
    rows = 64
    at_mine = pl.multiple_of(core[0] * 32, 32)
    at_other = pl.multiple_of(32 - core[0] * 32, 32)
    for l in range(LAYERS):
        rhs[l * rows : l * rows + 32] = mine[l]
        rhs[l * rows + 32 : l * rows + 64] = other[l]
    rhs[512:640] = g[...]
    rhs[640:768] = x[...]
    zero = jnp.zeros((rows, 128), BF)

    def block(l, p):
        if p < 2:
            return got[l % 4, l // 4, :, 256 + 128 * p : 384 + 128 * p]
        if l == 7:
            return got[0, 0, :, 128 * p : 128 * p + 128]
        return got[7 - l, 0, :, 384:512]

    acts, hs = [zero] * LAYERS, []
    for l in range(LAYERS):
        h = got[l % 4, l // 4, :, 0:128].astype(F32)
        pairs = range((l + 1) // 2)
        if len(pairs):
            left = jnp.concatenate([block(l, p) for p in pairs], axis=1)
            right = jnp.concatenate(acts[: 2 * len(pairs)], axis=0)
            h = h + mm(left, right)
        hs.append(h)
        acts[l] = (h * (1.0 / (1.0 + jnp.exp(-h)))).astype(BF)

    turned = {}
    for p in range(4):
        for q in range(p, 4):
            upper = zero if p == q else block(2 * q, p)
            both = jnp.concatenate([upper, block(2 * q + 1, p)], axis=0)
            turned[p, q] = both.T
    deltas = [zero] * LAYERS
    for l in reversed(range(LAYERS)):
        e = got[l % 4, l // 4, :, 128:256].astype(F32)
        pairs = range((l + 1) // 2, 4)
        if len(pairs):
            lo = rows * (l % 2)
            left = jnp.concatenate([turned[l // 2, q][lo : lo + rows] for q in pairs], axis=1)
            right = jnp.concatenate(deltas[2 * pairs[0] :], axis=0)
            e = e + mm(left, right)
        s = 1.0 / (1.0 + jnp.exp(-hs[l]))
        deltas[l] = (e * (s * (1.0 + hs[l] * (1.0 - s)))).astype(BF)

    act = jnp.concatenate(acts, axis=0)
    delta = jnp.concatenate(deltas, axis=0)
    row_layer = lax.broadcasted_iota(jnp.int32, (128, 128), 0) // rows
    col_layer = lax.broadcasted_iota(jnp.int32, (128, 128), 1) // rows
    cross = []
    for p in range(4):
        at, end = 128 * p, 128 * p + 128
        before = mm_nt(delta[at:end], act[:end])
        after = mm_nt(act[at:end], delta[at:])
        own = jnp.where(
            row_layer < col_layer, after[:, :128], jnp.where(row_layer > col_layer, before[:, at:end], 0.0)
        )
        sides = ([before[:, :at]] if p else []) + [own] + ([after[:, 128:]] if p < 3 else [])
        cross.append(jnp.concatenate(sides, axis=1).astype(BF))
    cross = jnp.concatenate(cross, axis=0)
    lhs = jnp.concatenate([cross, act, delta], axis=1)
    for n in range(4):
        cols = slice(256 * n, 256 * n + 256)
        grads = mm(lhs, rhs[:, cols]).astype(BF)
        for l in range(LAYERS):
            out[l, pl.ds(at_mine, 32), cols] = grads[rows * l : rows * l + 32]
            out[l, pl.ds(at_other, 32), cols] = grads[rows * l + 32 : rows * l + 64]


def pick(z, row, col, lane):
    sub = lax.broadcasted_iota(jnp.int32, (8, 128), 0)
    row = jnp.broadcast_to(row, (8, 128))
    col = jnp.broadcast_to(col + (lane // 32) % 2 * 64, (8, 128))
    first = jnp.broadcast_to(lane < 64, (8, 128))
    total = jnp.zeros((8, 128), F32)
    for r in range(8):
        left, right = (
            jnp.take_along_axis(
                z[8 * r : 8 * r + 8, 128 * u : 128 * u + 128], col, axis=1, mode="promise_in_bounds"
            )
            for u in range(2)
        )
        total = total + jnp.where(sub + 8 * r == row, jnp.where(first, left, right), 0.0)
    return jnp.sum(total, axis=0, keepdims=True)


def choose(field, keep, row_t, col_t, vals):
    lane = lax.broadcasted_iota(jnp.int32, (1, 128), 1)
    for s in range(8):
        piece = field(s)
        piece = jnp.concatenate([piece[:, 256 * q : 256 * q + 256] for q in range(4)], axis=0)
        if piece.dtype == BF:
            y = mm(jnp.concatenate([piece, piece], axis=1), col_t[256:768])
        else:
            y = by_cols(piece, col_t[...])
        for q in range(4):
            t = 4 * s + q
            z = by_rows(row_t[...], y[64 * q : 64 * q + 64])
            where = keep[t : t + 1, :]
            vals[t : t + 1, :] = pick(z, where // 64, where % 64, lane)


def past_kernel(momentum, keep, row_t, col_t, vals):
    choose(lambda s: DECAY * momentum[:, 1024 * s : 1024 * s + 1024].astype(F32), keep, row_t, col_t, vals)


def coef_kernel(grad, past, keep, row_t, col_t, vals, sent):
    choose(lambda s: grad[s], keep, row_t, col_t, vals)
    value = vals[...] + past[...]
    vals[...] = value
    where = keep[...].astype(F32)
    first = lax.broadcasted_iota(jnp.int32, (32, 128), 1) < 64
    sent[0:32, :] = jnp.where(first, value, pltpu.roll(where, 64, 1))
    sent[32:64, :] = jnp.where(first, pltpu.roll(value, 64, 1), where)


def half_kernel(core, weight, out, sems):
    at = pl.multiple_of(core[0] * 32, 32)
    copies = [
        pltpu.make_async_copy(weight.at[pl.ds(at, 32), pl.ds(1024 * s, 1024)], out.at[s], sems.at[s])
        for s in range(LAYERS)
    ]
    for copy in copies:
        copy.start()
    for copy in copies:
        copy.wait()


def rest_kernel(vals, keep, momentum, grad, row_t, col_t, out):
    lane = lax.broadcasted_iota(jnp.int32, (1, 128), 1)
    row_id = lax.broadcasted_iota(jnp.int32, (64, 128), 0)
    col_id = lax.broadcasted_iota(jnp.int32, (256, 128), 0)
    for s in range(8):
        parts = []
        for q in range(4):
            t = 4 * s + q
            where = keep[t : t + 1, :]
            spread = jnp.where(row_id == where // 64, vals[t : t + 1, :], 0.0)
            col_hot = jnp.where(col_id == where % 64 + lane // 32 * 64, 1.0, 0.0).astype(BF)
            both = mm_nt(jnp.concatenate(split(spread), axis=0), col_hot)
            parts.append(by_rows(row_t[...], both[0:64] + both[64:128]))
        y = by_cols(jnp.concatenate(parts, axis=0), col_t[...])
        for q in range(4):
            at = 256 * q
            cols = slice(1024 * s + at, 1024 * s + at + 256)
            fresh = DECAY * momentum[:, cols].astype(F32) + grad[s, :, at : at + 256].astype(F32)
            out[:, cols] = (fresh - y[64 * q : 64 * q + 64]).astype(BF)


def owner_kernel(seen, row_t, col_t, out):
    lane = lax.broadcasted_iota(jnp.int32, (32, 128), 1)
    top, bottom = seen[0:32, :], seen[32:64, :]
    value = jnp.where(lane < 64, top, pltpu.roll(bottom, 64, 1))
    where = jnp.where(lane < 64, pltpu.roll(top, 64, 1), bottom).astype(jnp.int32)
    row = where // 64
    col = where % 64 + (lane // 32) % 2 * 64
    row_id = lax.broadcasted_iota(jnp.int32, (64, 128), 0)
    col_id = lax.broadcasted_iota(jnp.int32, (128, 128), 0)
    total = jnp.zeros((128, 128), F32)
    for t in range(0, 32, 2):
        lefts, rights = [], []
        for v in (t, t + 1):
            spread = jnp.where(row_id == row[v : v + 1, :], value[v : v + 1, :], 0.0)
            lefts.append(jnp.concatenate(split(spread), axis=0))
            rights.append(jnp.where(col_id == col[v : v + 1, :], 1.0, 0.0).astype(BF))
        total = total + mm_nt(jnp.concatenate(lefts, axis=1), jnp.concatenate(rights, axis=1))
    summed = total[0:64] + total[64:128]
    decoded = by_cols(by_rows(row_t[...], summed), col_t[...]).astype(BF)
    for m in range(out.shape[0]):
        out[m] = decoded


def level_kernel(part, far, out):
    total = (part[...].astype(F32) + far[...].astype(F32)).astype(BF)
    for i in range(4):
        out[i] = total


def place(core, blocks, out, sems):
    copies = []
    for m in range(32):
        owner = 2 * (m % 16) + core
        at = pl.multiple_of(owner * 256 + 128 * (m // 16), 128)
        copies.append(pltpu.make_async_copy(blocks.at[m], out.at[:, pl.ds(at, 128)], sems.at[m]))
    for copy in copies:
        copy.start()
    for copy in copies:
        copy.wait()


def early_kernel(core, here, out, sems):
    place(core[0], here, out, sems)


def join_kernel(core, there, begun, out, sems):
    place(1 - core[0], there, out, sems)


def call(kernel, out_shape, in_specs, args, scratch=(), flops=0, space=pltpu.VMEM, alias=None):
    outs = jax.tree.map(lambda _: pl.BlockSpec(memory_space=space), out_shape)
    return pl.pallas_call(
        kernel,
        out_shape=out_shape,
        in_specs=in_specs,
        out_specs=outs,
        scratch_shapes=list(scratch),
        input_output_aliases=alias or {},
        compiler_params=pltpu.CompilerParams(vmem_limit_bytes=32 * 1024 * 1024),
        cost_estimate=pl.CostEstimate(flops=flops, bytes_accessed=0, transcendentals=0),
    )(*args)


def step(inputs, cotangent, weights, momentum, keep_index):
    core = lax.axis_index("core").astype(jnp.int32)
    core_at = core.reshape(1)
    weight = weights[0]
    rows, width = weight.shape
    cols = width // LAYERS
    full = LAYERS * rows
    struct = jax.ShapeDtypeStruct

    half = call(
        half_kernel,
        struct((LAYERS, rows // 2, cols), BF),
        [SCALAR, pl.BlockSpec(memory_space=pltpu.HBM)],
        (core_at, weight),
        [pltpu.SemaphoreType.DMA((LAYERS,))],
        1000,
    )
    mine = a2a(half, S)
    other = swap_cores(mine)
    w = jnp.concatenate([mine, other], axis=1).reshape(full, cols)

    both = jnp.concatenate([inputs, cotangent], axis=0)
    proj = [mm_nt(v.reshape(full // 2, cols), both).astype(BF).reshape(LAYERS, rows // 2, 256) for v in (mine, other)]
    proj = jnp.concatenate(proj, axis=1)
    gram = mm_nt(w, w).astype(BF).reshape(LAYERS, rows, full)
    packed = (
        [gram[7, :, 256:]]
        + [jnp.concatenate([gram[l, :, :128], gram[7 - l, :, 256:384]], axis=1) for l in (1, 2)]
        + [gram[l, :, :256] for l in range(3, LAYERS)]
    )
    chunks = [jnp.concatenate([proj[l], packed[l]], axis=1) for l in range(LAYERS)]
    payload = jnp.stack([jnp.stack([chunks[x], chunks[x + 4]]) for x in range(4)])
    part = jnp.sum(a2a(payload, "x").astype(F32), axis=0).astype(BF)
    far = lax.ppermute(part, "zh", [(0, 1), (1, 0)])
    got = call(level_kernel, struct((4, 2, rows, full), BF), whole(2), (part, far))
    got = a2a(got, "x")

    grads = call(
        relay_kernel,
        struct((LAYERS, rows, cols), BF),
        [SCALAR] + whole(5),
        (core_at, got, inputs, cotangent, mine, other),
        [pltpu.VMEM((768, cols), BF)],
        2 * 512 * 768 * 1024,
    )
    grad = a2a(grads, S)

    basis = dct_tables()
    keep = keep_index[0, 0].reshape(32, 128)
    values = struct((32, 128), F32)
    tables = (row_table(basis), col_table(basis.T, 4))
    flops = 2 * 2048 * 768 * 256
    past = call(past_kernel, values, whole(4), (momentum[0, 0], keep) + tables, (), flops)
    vals, sent = call(coef_kernel, (values, struct((64, 128), F32)), whole(5), (grad, past, keep) + tables, (), flops)
    seen = a2a(sent, DP)
    momentum_out = call(
        rest_kernel,
        struct((rows, width), BF),
        whole(6),
        (vals, keep, momentum[0, 0], grad, row_table(basis.T), col_table(basis, 4)),
        (),
        2 * 2048 * 768 * 256 * 4,
    )

    spread = call(
        owner_kernel,
        struct((32, 64, 128), BF),
        whole(3),
        (seen, row_table(basis.T), col_table(basis, 2)),
        (),
        2 * 64 * 128 * 4096,
    )
    here = a2a(spread, CHIP)
    there = swap_cores(here)
    sems = [pltpu.SemaphoreType.DMA((32,))]
    shape = struct((rows, width), BF)
    hbm = pl.BlockSpec(memory_space=pltpu.HBM)
    update = call(early_kernel, shape, [SCALAR] + whole(1), (core_at, here), sems, 1000, pltpu.HBM)
    update = call(
        join_kernel, shape, [SCALAR] + whole(1) + [hbm], (core_at, there, update), sems, 1000, pltpu.HBM, {2: 0}
    )
    return (momentum_out[None, None], update[None, None])


def solution(mesh):
    fine = Mesh(mesh.devices.reshape(2, 4, 4, 8, 2), ("zh", "x", "zl", "y", "core"))
    return jax.shard_map(
        step,
        mesh=fine,
        in_specs=(
            P(DP, S),
            P(DP, S),
            P(S, None, None),
            P(S, DP, None, None),
            P(S, DP, None, None),
        ),
        out_specs=(P(S, DP, None, None), P(S, DP, None, None)),
        check_vma=False,
    )
```
